32 devices in a mesh: leaf: 4 (over y, core), grid: 8 (over z, x).
Axes of the slice: x: 2, y: 2, z: 4, core: 2. Of those that a mesh axis runs over, the one named last changes fastest.
Arguments:
- ainv_sep: bfloat16 [4, 2048, 2048], P('leaf', 'grid'), may hold values from -6 to 6
- l_panel: bfloat16 [4, 2048, 512], P('leaf', 'grid'), may hold values from -0.125 to 0.125
- block_mask: int32 [4, 1, 4], P('leaf'), may hold values 0 or 1
- owner: int32 [4, 4], P('leaf'), may hold values 0 or 1
- dinv: float32 [4, 512, 512], P('leaf', 'grid'), may hold values from -6 to 6
Outputs:
- ainv_panel: bfloat16 [4, 2048, 512], P('leaf', 'grid')
- ainv_upper: bfloat16 [4, 512, 2048], P('leaf', 'grid')
- ainv_diag: float32 [4, 512, 512], P('leaf', 'grid')
The draws below stay inside these ranges and needn't reach their ends.
All inputs are finite; a program needn't handle non-finite values. No bound on the sum of `block_mask` or of `owner` on one device may be relied on, other than what follows from the above.
Results may differ from the reference program's by a relative error of at most 0.0019.
Values may be sent and summed in bfloat16 or wider, within the bound.
A program may use at most 128 MiB of HBM per device.

```python
import jax
import jax.numpy as jnp
from jax import lax

B = 512
NSUP = 1
SEP = 2048
NB = 4
W = 512
N_LEAF = 4


def with_ends(drawn, key, least, high):
    place = [jax.random.randint(jax.random.fold_in(key, axis), (), 0, length) for axis, length in enumerate(drawn.shape)]
    longest = drawn.shape.index(max(drawn.shape))
    beside = place[:longest] + [(place[longest] + 1) % drawn.shape[longest]] + place[longest + 1:]
    return drawn.at[tuple(place)].set(least).at[tuple(beside)].set(high)


def shard_levels(rng, shape, split, least, largest):
    level, own = 1.0, jax.random.fold_in(rng, 6)
    for position, parts in split:
        draws = jnp.exp(jax.random.uniform(jax.random.fold_in(own, position), (parts,), jnp.float32, least / len(split), largest / len(split)))
        level = level * jnp.repeat(draws, shape[position] // parts).reshape([-1 if axis == position else 1 for axis in range(len(shape))])
    return level


def normal_values(rng, shape, deviation, limit, pieces=(), dtype=jnp.bfloat16):
    array = deviation * jax.random.normal(rng, shape, jnp.float32)
    if pieces:
        array = array * shard_levels(rng, shape, pieces, -0.22, 0.18)
    return jnp.clip(array, -limit, limit).astype(dtype)


def setup_inputs(seed: int = 0) -> dict:
    key_list = jax.random.split(jax.random.key(seed), 6)
    ainv_sep = normal_values(key_list[0], (N_LEAF, SEP, SEP), 1.0, 6.0, ((0, 4), (1, 8)))
    l_panel = normal_values(key_list[1], (N_LEAF, SEP, W), SEP ** -0.5, 0.125, ((0, 4), (1, 8)))
    block_mask = with_ends((jax.random.randint(key_list[2], (N_LEAF, NSUP, NB), 0, 3) < 2).astype(jnp.int32), jax.random.fold_in(key_list[2], 1), 0, 1)
    owner = with_ends((jax.random.randint(key_list[3], (N_LEAF, NB), 0, 2) < 1).astype(jnp.int32), jax.random.fold_in(key_list[3], 1), 0, 1)
    dinv = normal_values(key_list[4], (N_LEAF, W, B), 1.0, 6.0, ((0, 4), (1, 8)), jnp.float32)
    return dict(ainv_sep=ainv_sep, l_panel=l_panel, block_mask=block_mask, owner=owner, dinv=dinv)


def reference(ainv_sep, l_panel, block_mask, owner, dinv):
    panels = []
    uppers = []
    diags = []
    for group in range(N_LEAF):
        own_block = ainv_sep[group].astype(jnp.float32)
        sibling = ainv_sep[group ^ 1].astype(jnp.float32)
        colmask = jnp.repeat(owner[group], B)
        mixed = jnp.where(colmask[None, :] == 1, sibling, own_block)
        rowmask = jnp.repeat(jnp.repeat(block_mask[group].T, B, axis=0), B, axis=1)
        masked = jnp.where(rowmask == 1, l_panel[group], jnp.zeros((), jnp.bfloat16)).astype(jnp.float32)
        panel = (-jnp.dot(mixed, masked, precision=lax.Precision.HIGHEST)).astype(jnp.bfloat16)
        panels.append(panel)
        uppers.append(panel.T)
        panel_f = panel.astype(jnp.float32).reshape(SEP, NSUP, B)
        masked_f = masked.reshape(SEP, NSUP, B)
        update = jnp.einsum("ski,skc->kic", panel_f, masked_f, precision=lax.Precision.HIGHEST)
        diags.append(dinv[group] - update.reshape(NSUP * B, B))
    return jnp.stack(panels), jnp.stack(uppers), jnp.stack(diags)
```

```python
import functools

import jax
import jax.numpy as jnp
from jax import lax
from jax.experimental import pallas as pl
from jax.experimental.pallas import tpu as pltpu
from jax.sharding import PartitionSpec as P

B = 512
MESH = pl.DeviceIdType.MESH
FULL_K = 2048


def kernel(
    n, slices, mask_ref, owner_ref, ainv_ref, lp_ref, dinv_ref,
    panel_ref, upper_ref, diag_ref,
    sib, whole, flipped,
    sib_send, sib_recv, x_send, up_send, down_send, recv, flip_send, flip_recv,
):
    leaf, me = lax.axis_index("leaf"), lax.axis_index("grid")
    z, x = lax.div(me, 2), lax.rem(me, 2)
    line = n // 2
    partner = 2 * z + (1 - x)
    above, below = jnp.minimum(me + 2, n - 1), jnp.maximum(me - 2, 0)
    has_up, has_down = z < line - 1, z > 0
    sibling = leaf + 1 - 2 * lax.rem(leaf, 2)
    rows, depth = ainv_ref.shape[1], ainv_ref.shape[2]
    width = lp_ref.shape[2]
    cols = width // slices
    out_rows = dinv_ref.shape[1]
    per_slice = cols // out_rows
    balance = line >= 4

    barrier = pltpu.get_barrier_semaphore()

    def greet(where):
        pl.semaphore_signal(barrier, inc=1, device_id=where, device_id_type=MESH)

    greet((sibling, me))
    greet((leaf, partner))

    @pl.when(has_up)
    def _():
        greet((leaf, above))

    @pl.when(has_down)
    def _():
        greet((leaf, below))

    pl.semaphore_wait(barrier, 4 - (z == 0).astype(jnp.int32) - (z == line - 1).astype(jnp.int32))

    def part(ref, j, h):
        start = j * rows if isinstance(j, int) else pl.multiple_of(j * rows, rows)
        return ref.at[pl.ds(start, rows), pl.ds(h * cols, cols)]

    def send(j, h, sems, to, mine=False):
        src = lp_ref.at[0, :, pl.ds(h * cols, cols)] if mine else part(whole, j, h)
        return pltpu.make_async_remote_copy(
            src_ref=src, dst_ref=part(whole, j, h), send_sem=sems.at[j, h],
            recv_sem=recv.at[j, h], device_id=(leaf, to), device_id_type=MESH)

    def arrived(j, h):
        pltpu.make_async_remote_copy(
            src_ref=part(whole, j, h), dst_ref=part(whole, j, h), send_sem=x_send.at[j, h],
            recv_sem=recv.at[j, h], device_id=(leaf, partner), device_id_type=MESH).wait_recv()

    def half(h):
        return h % 2 == 0

    def moved_below(d, h):
        if not balance or d != 1:
            return False
        return (z == 1) | (z == line - 1) if half(h) else z == 1

    def moved_above(d, h):
        if not balance or d != 1:
            return False
        return (z == line - 2) | (z == 0) if half(h) else z == line - 2

    def turn_up(h):
        return (z == 0) | (z == line - 2) if half(h) else z == 0

    def turn_down(h):
        return (z == line - 1) | (z == 1) if half(h) else z == line - 1

    def own(h, act):
        act(send(me, h, x_send, partner, True))

        @pl.when(has_up)
        def _():
            act(send(me, h, up_send, above, True))

        @pl.when(has_down)
        def _():
            act(send(me, h, down_send, below, True))

    def turn(h, act):
        if not balance:
            return

        @pl.when(turn_up(h))
        def _():
            act(send(partner, h, up_send, above))

        @pl.when(turn_down(h))
        def _():
            act(send(partner, h, down_send, below))

    def relay_up(h, d, act, wait):
        j = me - 2 * d

        @pl.when(z - d >= 0)
        def _():
            if wait:
                arrived(j, h)

            @pl.when(has_up)
            def _():
                act(send(j, h, up_send, above))

            @pl.when(jnp.logical_not(moved_below(d, h)))
            def _():
                act(send(j, h, x_send, partner))

    def relay_down(h, d, act, wait):
        j = me + 2 * d

        @pl.when(z + d < line)
        def _():
            if wait:
                arrived(j, h)

            @pl.when(has_down)
            def _():
                act(send(j, h, down_send, below))

            @pl.when(jnp.logical_not(moved_above(d, h)))
            def _():
                act(send(j, h, x_send, partner))

    start, done = (lambda c: c.start()), (lambda c: c.wait_send())

    def flip(d):
        return pltpu.make_async_remote_copy(
            src_ref=flipped.at[d], dst_ref=upper_ref.at[0, :, pl.ds(pl.multiple_of(me * rows, rows), rows)],
            send_sem=flip_send.at[d], recv_sem=flip_recv.at[me],
            device_id=(leaf, d), device_id_type=MESH)

    swap = pltpu.make_async_remote_copy(
        src_ref=ainv_ref.at[0], dst_ref=sib, send_sem=sib_send, recv_sem=sib_recv,
        device_id=(sibling, me), device_id_type=MESH)

    tile = min(FULL_K, depth)

    def product(left, h):
        def step(i, total):
            k = pl.ds(pl.multiple_of(i * tile, tile), tile)
            return total + jnp.dot(left[:, k], whole[k, pl.ds(h * cols, cols)],
                                   preferred_element_type=jnp.float32)
        if depth == tile:
            return jnp.dot(left[...], whole[:, pl.ds(h * cols, cols)],
                           preferred_element_type=jnp.float32)
        return lax.fori_loop(0, depth // tile, step, jnp.zeros((rows, cols), jnp.float32))

    def finish(h):
        for d in range(1, line):
            @pl.when(z - d >= 0)
            def _():
                arrived(partner - 2 * d, h)

            @pl.when(z + d < line)
            def _():
                arrived(partner + 2 * d, h)
        panel = (-product(sib, h)).astype(jnp.bfloat16)
        turned = panel.astype(jnp.float32).T.reshape(per_slice, out_rows, rows)
        flipped[pl.ds(h * per_slice, per_slice)] = turned.astype(jnp.bfloat16)
        panel_ref[0, :, pl.ds(h * cols, cols)] = panel
        for d in range(h * per_slice, (h + 1) * per_slice):
            @pl.when(me != d)
            def _():
                flip(d).start()

            @pl.when(me == d)
            def _():
                upper_ref[0, :, pl.ds(pl.multiple_of(me * rows, rows), rows)] = flipped[d]

    order = list(range(slices))
    if slices > 2:
        order = [0, slices - 1] + list(range(1, slices - 1))

    own(order[0], start)
    if slices > 1:
        own(order[1], start)
    swap.start()
    whole[pl.ds(pl.multiple_of(me * rows, rows), rows), :] = lp_ref[0]

    for step in range(1, slices + line - 1):
        for d in range(1, line):
            i = step - d
            if not 0 <= i < slices:
                continue
            h = order[i]
            if d == 1:
                arrived(partner, h)
                turn(h, start)
            relay_up(h, d, start, True)
            relay_down(h, d, start, True)
        if step + 1 < slices:
            own(order[step + 1], start)
        if step == 1:
            swap.wait_recv()

            def mix(b, carry):
                k = pl.ds(pl.multiple_of(b * B, B), B)
                kept = jnp.where(owner_ref[0, b] == 1, sib[:, k], ainv_ref[0, :, k])
                sib[:, k] = jnp.where(mask_ref[0, 0, b] == 1, kept, jnp.zeros_like(kept))
                return carry

            lax.fori_loop(0, depth // B, mix, 0)
        i = step - (line - 1)
        if 0 <= i < slices:
            finish(order[i])

    for j in range(n):
        @pl.when(me != j)
        def _():
            pltpu.make_async_remote_copy(
                src_ref=flipped.at[0], dst_ref=upper_ref.at[0, :, pl.ds(j * rows, rows)],
                send_sem=flip_send.at[0], recv_sem=flip_recv.at[j],
                device_id=(leaf, partner), device_id_type=MESH).wait_recv()

    def update(b, total):
        k = pl.ds(pl.multiple_of(b * B, B), B)
        u = upper_ref[0, :, k]
        u = jnp.where(mask_ref[0, 0, b] == 1, u, jnp.zeros_like(u))
        return total - jnp.dot(u, whole[k, :], preferred_element_type=jnp.float32)

    diag_ref[0] = lax.fori_loop(0, depth // B, update, dinv_ref[0], unroll=depth <= tile)

    swap.wait_send()
    for h in range(slices):
        own(h, done)
        turn(h, done)
        for d in range(1, line):
            relay_up(h, d, done, False)
            relay_down(h, d, done, False)
    for d in range(n):
        @pl.when(me != d)
        def _():
            flip(d).wait_send()


def solution(mesh):
    n = mesh.shape["grid"]
    slices = 4 if n <= 16 else 1

    def body(ainv_sep, l_panel, block_mask, owner, dinv):
        rows, depth = ainv_sep.shape[1:]
        width = l_panel.shape[2]
        out_rows = dinv.shape[1]
        vmem = pl.BlockSpec(memory_space=pltpu.VMEM)
        smem = pl.BlockSpec(memory_space=pltpu.SMEM)
        dma = pltpu.SemaphoreType.DMA
        return pl.pallas_call(
            functools.partial(kernel, n, slices),
            out_shape=(
                jax.ShapeDtypeStruct((1, rows, width), jnp.bfloat16),
                jax.ShapeDtypeStruct((1, out_rows, depth), jnp.bfloat16),
                jax.ShapeDtypeStruct((1, out_rows, width), jnp.float32),
            ),
            in_specs=[smem, smem, vmem, vmem, vmem],
            out_specs=(vmem, vmem, vmem),
            scratch_shapes=[
                pltpu.VMEM((rows, depth), jnp.bfloat16),
                pltpu.VMEM((depth, width), jnp.bfloat16),
                pltpu.VMEM((n, out_rows, rows), jnp.bfloat16),
                dma, dma,
                dma((n, slices)), dma((n, slices)), dma((n, slices)), dma((n, slices)),
                dma((n,)), dma((n,)),
            ],
            compiler_params=pltpu.CompilerParams(collective_id=0, has_side_effects=True),
        )(block_mask, owner, ainv_sep, l_panel, dinv)

    placed = (
        P("leaf", "grid", None),
        P("leaf", "grid", None),
        P("leaf", None, None),
        P("leaf", None),
        P("leaf", "grid", None),
    )
    return jax.shard_map(
        body,
        mesh=mesh,
        in_specs=placed,
        out_specs=(P("leaf", "grid", None), P("leaf", "grid", None), P("leaf", "grid", None)),
        check_vma=False,
    )
```

```python
import functools

import jax
import jax.numpy as jnp
from jax import lax
from jax.experimental import pallas as pl
from jax.experimental.pallas import tpu as pltpu
from jax.sharding import PartitionSpec as P

B = 512
MESH = pl.DeviceIdType.MESH
FULL_K = 2048


def kernel(
    n, slices, mask_ref, owner_ref, ainv_ref, lp_ref, dinv_ref,
    panel_ref, upper_ref, diag_ref,
    sib, held, whole, flipped, masked,
    sib_send, sib_recv, x_send, up_send, down_send, recv, flip_send, flip_recv,
    load_sem, keep_sem,
):
    leaf, me = lax.axis_index("leaf"), lax.axis_index("grid")
    z, x = lax.div(me, 2), lax.rem(me, 2)
    line = n // 2
    partner = 2 * z + (1 - x)
    above, below = jnp.minimum(me + 2, n - 1), jnp.maximum(me - 2, 0)
    has_up, has_down = z < line - 1, z > 0
    sibling = leaf + 1 - 2 * lax.rem(leaf, 2)
    rows, depth = ainv_ref.shape[1], ainv_ref.shape[2]
    width = lp_ref.shape[2]
    cols = width // slices
    out_rows = dinv_ref.shape[1]
    per_slice = cols // out_rows
    balance = False

    def part(ref, j, h):
        return ref.at[j, h]

    barrier = pltpu.get_barrier_semaphore()

    def greet(where):
        pl.semaphore_signal(barrier, inc=1, device_id=where, device_id_type=MESH)

    greet((sibling, me))
    greet((leaf, partner))

    @pl.when(has_up)
    def _():
        greet((leaf, above))

    @pl.when(has_down)
    def _():
        greet((leaf, below))

    def load(h):
        return pltpu.make_async_copy(
            lp_ref.at[0, :, pl.ds(h * cols, cols)], part(whole, me, h), load_sem.at[h])

    for h in range(slices):
        load(h).start()
    keep = pltpu.make_async_copy(ainv_ref.at[0], held, keep_sem)
    keep.start()
    pl.semaphore_wait(barrier, 4 - (z == 0).astype(jnp.int32) - (z == line - 1).astype(jnp.int32))

    def send(j, h, sems, to):
        return pltpu.make_async_remote_copy(
            src_ref=part(whole, j, h), dst_ref=part(whole, j, h), send_sem=sems.at[j, h],
            recv_sem=recv.at[j, h], device_id=(leaf, to), device_id_type=MESH)

    def arrived(j, h):
        pltpu.make_async_remote_copy(
            src_ref=part(whole, j, h), dst_ref=part(whole, j, h), send_sem=x_send.at[j, h],
            recv_sem=recv.at[j, h], device_id=(leaf, partner), device_id_type=MESH).wait_recv()

    def half(h):
        return h % 2 == 0

    def moved_below(d, h):
        if not balance or d != 1:
            return False
        return (z == 1) | (z == line - 1) if half(h) else z == 1

    def moved_above(d, h):
        if not balance or d != 1:
            return False
        return (z == line - 2) | (z == 0) if half(h) else z == line - 2

    def turn_up(h):
        return (z == 0) | (z == line - 2) if half(h) else z == 0

    def turn_down(h):
        return (z == line - 1) | (z == 1) if half(h) else z == line - 1

    def own(h, act):
        act(send(me, h, x_send, partner))

        @pl.when(has_up)
        def _():
            act(send(me, h, up_send, above))

        @pl.when(has_down)
        def _():
            act(send(me, h, down_send, below))

    def turn(h, act):
        if not balance:
            return

        @pl.when(turn_up(h))
        def _():
            act(send(partner, h, up_send, above))

        @pl.when(turn_down(h))
        def _():
            act(send(partner, h, down_send, below))

    def relay_up(h, d, act, wait):
        j = me - 2 * d

        @pl.when(z - d >= 0)
        def _():
            if wait:
                arrived(j, h)

            @pl.when(has_up)
            def _():
                act(send(j, h, up_send, above))

            @pl.when(jnp.logical_not(moved_below(d, h)))
            def _():
                act(send(j, h, x_send, partner))

    def relay_down(h, d, act, wait):
        j = me + 2 * d

        @pl.when(z + d < line)
        def _():
            if wait:
                arrived(j, h)

            @pl.when(has_down)
            def _():
                act(send(j, h, down_send, below))

            @pl.when(jnp.logical_not(moved_above(d, h)))
            def _():
                act(send(j, h, x_send, partner))

    start, done = (lambda c: c.start()), (lambda c: c.wait_send())

    def flip(d):
        return pltpu.make_async_remote_copy(
            src_ref=flipped.at[d], dst_ref=upper_ref.at[0, :, pl.ds(pl.multiple_of(me * rows, rows), rows)],
            send_sem=flip_send.at[d], recv_sem=flip_recv.at[me],
            device_id=(leaf, d), device_id_type=MESH)

    swap = pltpu.make_async_remote_copy(
        src_ref=ainv_ref.at[0], dst_ref=sib, send_sem=sib_send, recv_sem=sib_recv,
        device_id=(sibling, me), device_id_type=MESH)

    tile = min(FULL_K // rows, n)

    def columns(i, h):
        block = whole[pl.ds(i * tile, tile), h]
        return block.reshape(tile * rows, cols)

    def across(left, h, total):
        def step(i, total):
            k = pl.ds(pl.multiple_of(i * (tile * rows), tile * rows), tile * rows)
            return total + jnp.dot(left[:, k], columns(i, h), preferred_element_type=jnp.float32)

        if tile == n:
            return step(0, total)
        return lax.fori_loop(0, n // tile, step, total)

    def finish(h):
        for d in range(1, line):
            @pl.when(z - d >= 0)
            def _():
                arrived(partner - 2 * d, h)

            @pl.when(z + d < line)
            def _():
                arrived(partner + 2 * d, h)
        panel = (-across(sib, h, jnp.zeros((rows, cols), jnp.float32))).astype(jnp.bfloat16)
        turned = panel.astype(jnp.float32).T.reshape(per_slice, out_rows, rows)
        flipped[pl.ds(h * per_slice, per_slice)] = turned.astype(jnp.bfloat16)
        panel_ref[0, :, pl.ds(h * cols, cols)] = panel
        for d in range(h * per_slice, (h + 1) * per_slice):
            @pl.when(me != d)
            def _():
                flip(d).start()

            @pl.when(me == d)
            def _():
                upper_ref[0, :, pl.ds(pl.multiple_of(me * rows, rows), rows)] = flipped[d]

    order = list(range(slices))
    if slices > 2:
        order = [0, slices - 1] + list(range(1, slices - 1))

    for h in order:
        load(h).wait()
        own(h, start)
    swap.start()

    for d in range(1, line):
        for h in order:
            if d == 1:
                arrived(partner, h)
                turn(h, start)
            relay_up(h, d, start, True)
            relay_down(h, d, start, True)

    swap.wait_recv()
    keep.wait()

    def mix(b, carry):
        k = pl.ds(pl.multiple_of(b * B, B), B)
        kept = jnp.where(owner_ref[0, b] == 1, sib[:, k], held[:, k])
        sib[:, k] = jnp.where(mask_ref[0, 0, b] == 1, kept, jnp.zeros_like(kept))
        return carry

    lax.fori_loop(0, depth // B, mix, 0)
    for h in order:
        finish(h)

    for j in range(n):
        @pl.when(me != j)
        def _():
            pltpu.make_async_remote_copy(
                src_ref=flipped.at[0], dst_ref=upper_ref.at[0, :, pl.ds(j * rows, rows)],
                send_sem=flip_send.at[0], recv_sem=flip_recv.at[j],
                device_id=(leaf, partner), device_id_type=MESH).wait_recv()

    def sift(b, carry):
        k = pl.ds(pl.multiple_of(b * B, B), B)
        u = upper_ref[0, :, k]
        masked[:, k] = jnp.where(mask_ref[0, 0, b] == 1, u, jnp.zeros_like(u))
        return carry

    lax.fori_loop(0, depth // B, sift, 0)
    for h in range(slices):
        c = pl.ds(h * cols, cols)
        update = across(masked, h, jnp.zeros((out_rows, cols), jnp.float32))
        diag_ref[0, :, c] = dinv_ref[0, :, c] - update

    swap.wait_send()
    for h in range(slices):
        own(h, done)
        turn(h, done)
        for d in range(1, line):
            relay_up(h, d, done, False)
            relay_down(h, d, done, False)
    for d in range(n):
        @pl.when(me != d)
        def _():
            flip(d).wait_send()


def write_out(panel, upper, diag, panel_out, upper_out, diag_out, *sems):
    copies = [
        pltpu.make_async_copy(src, dst, sem)
        for src, dst, sem in zip((panel, upper, diag), (panel_out, upper_out, diag_out), sems)
    ]
    for copy in copies:
        copy.start()
    for copy in copies:
        copy.wait()


def solution(mesh):
    n = mesh.shape["grid"]
    slices = 4 if n <= 16 else 1

    def body(ainv_sep, l_panel, block_mask, owner, dinv):
        rows, depth = ainv_sep.shape[1:]
        width = l_panel.shape[2]
        out_rows = dinv.shape[1]
        vmem = pl.BlockSpec(memory_space=pltpu.VMEM)
        smem = pl.BlockSpec(memory_space=pltpu.SMEM)
        hbm = pl.BlockSpec(memory_space=pl.ANY)
        dma = pltpu.SemaphoreType.DMA
        results = pl.pallas_call(
            functools.partial(kernel, n, slices),
            out_shape=(
                pltpu.VMEM((1, rows, width), jnp.bfloat16),
                pltpu.VMEM((1, out_rows, depth), jnp.bfloat16),
                pltpu.VMEM((1, out_rows, width), jnp.float32),
            ),
            in_specs=[smem, smem, hbm, hbm, vmem],
            out_specs=(vmem, vmem, vmem),
            scratch_shapes=[
                pltpu.VMEM((rows, depth), jnp.bfloat16),
                pltpu.VMEM((rows, depth), jnp.bfloat16),
                pltpu.VMEM((n, slices, rows, width // slices), jnp.bfloat16),
                pltpu.VMEM((n, out_rows, rows), jnp.bfloat16),
                pltpu.VMEM((out_rows, depth), jnp.bfloat16),
                dma, dma,
                dma((n, slices)), dma((n, slices)), dma((n, slices)), dma((n, slices)),
                dma((n,)), dma((n,)),
                dma((slices,)), dma,
            ],
            compiler_params=pltpu.CompilerParams(collective_id=0, has_side_effects=True),
        )(block_mask, owner, ainv_sep, l_panel, dinv)
        return pl.pallas_call(
            write_out,
            out_shape=tuple(jax.ShapeDtypeStruct(r.shape, r.dtype) for r in results),
            in_specs=[vmem] * 3,
            out_specs=(hbm,) * 3,
            scratch_shapes=[dma, dma, dma],
        )(*results)

    placed = (
        P("leaf", "grid", None),
        P("leaf", "grid", None),
        P("leaf", None, None),
        P("leaf", None),
        P("leaf", "grid", None),
    )
    return jax.shard_map(
        body,
        mesh=mesh,
        in_specs=placed,
        out_specs=(P("leaf", "grid", None), P("leaf", "grid", None), P("leaf", "grid", None)),
        check_vma=False,
    )
```

```python
import functools

import jax
import jax.numpy as jnp
from jax import lax
from jax.experimental import pallas as pl
from jax.experimental.pallas import tpu as pltpu
from jax.sharding import PartitionSpec as P

B = 512
MESH = pl.DeviceIdType.MESH
FULL_K = 2048


def kernel(
    n, slices, mask_ref, owner_ref, ainv_ref, lp_ref, dinv_ref,
    panel_ref, upper_ref, diag_ref,
    sib, held, whole, flipped, masked,
    sib_send, sib_recv, x_send, up_send, down_send, recv, flip_send, flip_recv,
    load_sem, keep_sem, base, base_sem, mask, owners, mask_sem, owner_sem,
):
    leaf, me = lax.axis_index("leaf"), lax.axis_index("grid")
    z, x = lax.div(me, 2), lax.rem(me, 2)
    line = n // 2
    partner = 2 * z + (1 - x)
    above, below = jnp.minimum(me + 2, n - 1), jnp.maximum(me - 2, 0)
    has_up, has_down = z < line - 1, z > 0
    sibling = leaf + 1 - 2 * lax.rem(leaf, 2)
    rows, depth = ainv_ref.shape[1], ainv_ref.shape[2]
    width = lp_ref.shape[2]
    cols = width // slices
    out_rows = dinv_ref.shape[1]
    per_slice = cols // out_rows
    balance = line >= 4

    def part(ref, j, h):
        return ref.at[j, h]

    barrier = pltpu.get_barrier_semaphore()

    def greet(where):
        pl.semaphore_signal(barrier, inc=1, device_id=where, device_id_type=MESH)

    greet((sibling, me))
    greet((leaf, partner))

    @pl.when(has_up)
    def _():
        greet((leaf, above))

    @pl.when(has_down)
    def _():
        greet((leaf, below))

    def load(h):
        return pltpu.make_async_copy(
            lp_ref.at[0, :, pl.ds(h * cols, cols)], part(whole, me, h), load_sem.at[h])

    for h in range(slices):
        load(h).start()
    keep = pltpu.make_async_copy(ainv_ref.at[0], held, keep_sem)
    keep.start()
    initial = pltpu.make_async_copy(dinv_ref.at[0], base, base_sem)
    initial.start()
    flags = pltpu.make_async_copy(mask_ref, mask, mask_sem)
    flags.start()
    owned = pltpu.make_async_copy(owner_ref, owners, owner_sem)
    owned.start()
    pl.semaphore_wait(barrier, 4 - (z == 0).astype(jnp.int32) - (z == line - 1).astype(jnp.int32))

    def send(j, h, sems, to):
        return pltpu.make_async_remote_copy(
            src_ref=part(whole, j, h), dst_ref=part(whole, j, h), send_sem=sems.at[j, h],
            recv_sem=recv.at[j, h], device_id=(leaf, to), device_id_type=MESH)

    def arrived(j, h):
        pltpu.make_async_remote_copy(
            src_ref=part(whole, j, h), dst_ref=part(whole, j, h), send_sem=x_send.at[j, h],
            recv_sem=recv.at[j, h], device_id=(leaf, partner), device_id_type=MESH).wait_recv()

    def half(h):
        return h % 2 == 0

    def moved_below(d, h):
        if not balance or d != 1:
            return False
        return (z == 1) | (z == line - 1) if half(h) else z == 1

    def moved_above(d, h):
        if not balance or d != 1:
            return False
        return (z == line - 2) | (z == 0) if half(h) else z == line - 2

    def turn_up(h, early):
        if early:
            return z == 0
        return z == line - 2 if half(h) else None

    def turn_down(h, early):
        if early:
            return z == line - 1
        return z == 1 if half(h) else None

    def own(h, act):
        act(send(me, h, x_send, partner))

        @pl.when(has_up)
        def _():
            act(send(me, h, up_send, above))

        @pl.when(has_down)
        def _():
            act(send(me, h, down_send, below))

    def turn(h, act, early):
        if not balance or turn_up(h, early) is None:
            return

        @pl.when(turn_up(h, early))
        def _():
            act(send(partner, h, up_send, above))

        @pl.when(turn_down(h, early))
        def _():
            act(send(partner, h, down_send, below))

    def relay_up(h, d, act, wait):
        j = me - 2 * d

        @pl.when(z - d >= 0)
        def _():
            if wait:
                arrived(j, h)

            @pl.when(has_up)
            def _():
                act(send(j, h, up_send, above))

            @pl.when(jnp.logical_not(moved_below(d, h)))
            def _():
                act(send(j, h, x_send, partner))

    def relay_down(h, d, act, wait):
        j = me + 2 * d

        @pl.when(z + d < line)
        def _():
            if wait:
                arrived(j, h)

            @pl.when(has_down)
            def _():
                act(send(j, h, down_send, below))

            @pl.when(jnp.logical_not(moved_above(d, h)))
            def _():
                act(send(j, h, x_send, partner))

    start, done = (lambda c: c.start()), (lambda c: c.wait_send())

    def flip(d):
        return pltpu.make_async_remote_copy(
            src_ref=flipped.at[d], dst_ref=upper_ref.at[0, :, pl.ds(pl.multiple_of(me * rows, rows), rows)],
            send_sem=flip_send.at[d], recv_sem=flip_recv.at[me],
            device_id=(leaf, d), device_id_type=MESH)

    swap = pltpu.make_async_remote_copy(
        src_ref=ainv_ref.at[0], dst_ref=sib, send_sem=sib_send, recv_sem=sib_recv,
        device_id=(sibling, me), device_id_type=MESH)

    tile = min(FULL_K // rows, n)

    def columns(i, h):
        block = whole[pl.ds(i * tile, tile), h]
        return block.reshape(tile * rows, cols)

    def across(left, h, total):
        def step(i, total):
            k = pl.ds(pl.multiple_of(i * (tile * rows), tile * rows), tile * rows)
            return total + jnp.dot(left[:, k], columns(i, h), preferred_element_type=jnp.float32)

        if tile == n:
            return step(0, total)
        return lax.fori_loop(0, n // tile, step, total)

    def finish(h):
        for d in range(1, line):
            @pl.when(z - d >= 0)
            def _():
                arrived(partner - 2 * d, h)

            @pl.when(z + d < line)
            def _():
                arrived(partner + 2 * d, h)
        panel = (-across(sib, h, jnp.zeros((rows, cols), jnp.float32))).astype(jnp.bfloat16)
        turned = panel.astype(jnp.float32).T.reshape(per_slice, out_rows, rows)
        flipped[pl.ds(h * per_slice, per_slice)] = turned.astype(jnp.bfloat16)
        panel_ref[0, :, pl.ds(h * cols, cols)] = panel
        for d in range(h * per_slice, (h + 1) * per_slice):
            @pl.when(me != d)
            def _():
                flip(d).start()

            @pl.when(me == d)
            def _():
                upper_ref[0, :, pl.ds(pl.multiple_of(me * rows, rows), rows)] = flipped[d]

    order = list(range(slices))
    if slices > 2:
        order = [0, slices - 1] + list(range(1, slices - 1))

    for h in order:
        load(h).wait()
        own(h, start)
    swap.start()

    for d in range(1, line):
        for h in order:
            if d == 1:
                arrived(partner, h)
                turn(h, start, True)
            relay_up(h, d, start, True)
            relay_down(h, d, start, True)

    for h in order:
        turn(h, start, False)
    swap.wait_recv()
    keep.wait()
    initial.wait()
    flags.wait()
    owned.wait()

    def mix(b, carry):
        k = pl.ds(pl.multiple_of(b * B, B), B)
        kept = jnp.where(owners[0, b] == 1, sib[:, k], held[:, k])
        sib[:, k] = jnp.where(mask[0, 0, b] == 1, kept, jnp.zeros_like(kept))
        return carry

    lax.fori_loop(0, depth // B, mix, 0)
    for h in order:
        finish(h)

    for j in range(n):
        @pl.when(me != j)
        def _():
            pltpu.make_async_remote_copy(
                src_ref=flipped.at[0], dst_ref=upper_ref.at[0, :, pl.ds(j * rows, rows)],
                send_sem=flip_send.at[0], recv_sem=flip_recv.at[j],
                device_id=(leaf, partner), device_id_type=MESH).wait_recv()

    def sift(b, carry):
        k = pl.ds(pl.multiple_of(b * B, B), B)
        u = upper_ref[0, :, k]
        masked[:, k] = jnp.where(mask[0, 0, b] == 1, u, jnp.zeros_like(u))
        return carry

    lax.fori_loop(0, depth // B, sift, 0)
    for h in range(slices):
        c = pl.ds(h * cols, cols)
        update = across(masked, h, jnp.zeros((out_rows, cols), jnp.float32))
        diag_ref[0, :, c] = base[:, c] - update

    swap.wait_send()
    for h in range(slices):
        own(h, done)
        turn(h, done, True)
        turn(h, done, False)
        for d in range(1, line):
            relay_up(h, d, done, False)
            relay_down(h, d, done, False)
    for d in range(n):
        @pl.when(me != d)
        def _():
            flip(d).wait_send()


def solution(mesh):
    n = mesh.shape["grid"]
    slices = 4 if n <= 16 else 1

    def body(ainv_sep, l_panel, block_mask, owner, dinv):
        rows, depth = ainv_sep.shape[1:]
        width = l_panel.shape[2]
        out_rows = dinv.shape[1]
        vmem = pl.BlockSpec(memory_space=pltpu.VMEM)
        smem = pl.BlockSpec(memory_space=pltpu.SMEM)
        hbm = pl.BlockSpec(memory_space=pl.ANY)
        dma = pltpu.SemaphoreType.DMA
        results = pl.pallas_call(
            functools.partial(kernel, n, slices),
            out_shape=(
                pltpu.VMEM((1, rows, width), jnp.bfloat16),
                pltpu.VMEM((1, out_rows, depth), jnp.bfloat16),
                pltpu.VMEM((1, out_rows, width), jnp.float32),
            ),
            in_specs=[hbm] * 5,
            out_specs=(vmem, vmem, vmem),
            scratch_shapes=[
                pltpu.VMEM((rows, depth), jnp.bfloat16),
                pltpu.VMEM((rows, depth), jnp.bfloat16),
                pltpu.VMEM((n, slices, rows, width // slices), jnp.bfloat16),
                pltpu.VMEM((n, out_rows, rows), jnp.bfloat16),
                pltpu.VMEM((out_rows, depth), jnp.bfloat16),
                dma, dma,
                dma((n, slices)), dma((n, slices)), dma((n, slices)), dma((n, slices)),
                dma((n,)), dma((n,)),
                dma((slices,)), dma,
                pltpu.VMEM((out_rows, width), jnp.float32), dma,
                pltpu.SMEM(block_mask.shape, jnp.int32), pltpu.SMEM(owner.shape, jnp.int32), dma, dma,
            ],
            compiler_params=pltpu.CompilerParams(collective_id=0, has_side_effects=True),
        )(block_mask, owner, ainv_sep, l_panel, dinv)
        return tuple(results)

    placed = (
        P("leaf", "grid", None),
        P("leaf", "grid", None),
        P("leaf", None, None),
        P("leaf", None),
        P("leaf", "grid", None),
    )
    return jax.shard_map(
        body,
        mesh=mesh,
        in_specs=placed,
        out_specs=(P("leaf", "grid", None), P("leaf", "grid", None), P("leaf", "grid", None)),
        check_vma=False,
    )
```
